1024 devices in a mesh: dp: 8 (over z_hi, core), ctx: 128 (over x, y, z_lo).
Axes of the slice: x: 4, y: 4, z: 32 (z_hi: 4, z_lo: 8; z = z_hi * 8 + z_lo), core: 2. Of those that a mesh axis runs over, the one named last changes fastest.
Arguments:
- activations: bfloat16 [10240, 4096], P('ctx', 'dp'), may hold values from -6 to 6
- queries: bfloat16 [10240, 32, 128], P('ctx', 'dp'), may hold values from -300 to 300
- w_kv: bfloat16 [4096, 8, 2, 128], P(('dp', 'ctx')), may hold values from -0.09375 to 0.09375
- span_of: int32 [256], P('ctx'), may hold values from 0 to 255, as said below
Outputs:
- attended: bfloat16 [10240, 4096], P('ctx', 'dp')
The draws below stay inside these ranges and needn't reach their ends.
Inputs may be any that keep to these rules, and one draw needn't show every extreme that they name: `span_of`: each span number appears once. The two slots of one ctx index hold spans c and 2 * 128 - 1 - c for some c, in either order.
All inputs are finite; a program needn't handle non-finite values.
Results may differ from the reference program's by a relative error of at most 0.0066.
Values may be sent and summed in bfloat16 or wider, within the bound.
No kernel may reach another device: no remote copies, remote signals or barrier semaphores. Data moves between devices by JAX's collectives and lax.ppermute only.
A program may use at most 32 MiB of HBM per device.

```python
import math
import jax
import jax.numpy as jnp
from jax import lax

D = 4096
HD = 128
GROUP = 4
KV_HEADS = 8
Q_HEADS = 32
SPAN = 40
SEQ = 10240
N_CTX = 128


def span_table(key):
    pairs = jax.random.permutation(jax.random.fold_in(key, 201), N_CTX).astype(jnp.int32)
    flips = jax.random.randint(jax.random.fold_in(key, 202), (N_CTX,), 0, 2).astype(jnp.int32)
    upper = 2 * N_CTX - 1 - pairs
    first = jnp.where(flips == 1, upper, pairs)
    second = jnp.where(flips == 1, pairs, upper)
    return jnp.stack([first, second], axis=1).reshape(2 * N_CTX).astype(jnp.int32)


def base_inputs(key):
    inner = jax.random.fold_in(key, 101)
    return jnp.clip(jax.random.normal(inner, (SEQ, D), jnp.float32), -6.0, 6.0)


def base_w(key):
    inner = jax.random.fold_in(key, 102)
    raw = jnp.clip(jax.random.normal(inner, (D, KV_HEADS, 2, HD), jnp.float32), -6.0, 6.0)
    return raw * (1.0 / math.sqrt(D))


def draw_span_of(key, part):
    return span_table(key)


def draw_activations(key, part):
    return base_inputs(key).astype(jnp.bfloat16)


def draw_w_kv(key, part):
    return base_w(key).astype(jnp.bfloat16)


def draw_queries(key, part):
    inner = jax.random.fold_in(key, 103)
    query = jnp.clip(jax.random.normal(inner, (SEQ, Q_HEADS, HD), jnp.float32), -6.0, 6.0)
    return query.astype(jnp.bfloat16)


def setup_inputs(seed: int = 0) -> dict:
    key_of = jax.random.split(jax.random.key(seed), 5)
    activations = draw_activations(jax.random.fold_in(key_of[4], 71), 0)
    queries = draw_queries(jax.random.fold_in(key_of[4], 71), 0)
    w_kv = draw_w_kv(jax.random.fold_in(key_of[4], 71), 0)
    span_of = draw_span_of(jax.random.fold_in(key_of[4], 71), 0)
    return {"activations": activations, "queries": queries, "w_kv": w_kv, "span_of": span_of}


def reference(activations, queries, w_kv, span_of):
    rows = jnp.arange(SEQ, dtype=jnp.int32)
    position = (jnp.take(span_of, rows // SPAN) * SPAN + rows % SPAN).astype(jnp.int32)
    flat = w_kv.reshape(D, KV_HEADS * 2 * HD)
    key_value = jnp.dot(activations, flat, preferred_element_type=jnp.float32).astype(jnp.bfloat16)
    key_value = key_value.reshape(SEQ, KV_HEADS, 2, HD)
    visible = position[None, :] <= position[:, None]
    scale = 1.0 / math.sqrt(HD)

    def one_head(head):
        query = lax.dynamic_index_in_dim(queries, head, 1, keepdims=False).astype(jnp.float32)
        pair = lax.dynamic_index_in_dim(key_value, head // GROUP, 1, keepdims=False)
        keys = pair[:, 0].astype(jnp.float32)
        values = pair[:, 1]
        score = jnp.dot(query, keys.T, precision=lax.Precision.HIGHEST) * scale
        top = lax.optimization_barrier(jnp.max(jnp.where(visible, score, -1e+30), axis=1, keepdims=True))
        weight = jnp.where(visible, jnp.exp(score - top), 0.0)
        total = lax.optimization_barrier(jnp.sum(weight, axis=1, keepdims=True))
        mixed = jnp.dot(weight.astype(jnp.bfloat16), values, preferred_element_type=jnp.float32) / total
        return mixed.astype(jnp.bfloat16)
    heads_out = lax.map(one_head, jnp.arange(Q_HEADS, dtype=jnp.int32))
    return jnp.transpose(heads_out, (1, 0, 2)).reshape(SEQ, Q_HEADS * HD)
```

```python
import math

import jax
import jax.numpy as jnp
from jax import lax
from jax.experimental import pallas as pl
from jax.experimental.pallas import tpu as pltpu
from jax.sharding import Mesh
from jax.sharding import PartitionSpec as P


ROWS = ("x", "y", "zl")
HEADS = ("zh", "core")
PLANE = ("x", "y")
HIDDEN = -1e30
FLOOR = -1e29
STAT_ROWS = 16
SPAN_ROWS = 8


def shifted(value, axis, by):
    size = lax.axis_size(axis)
    return lax.ppermute(value, axis, [(i, (i + by) % size) for i in range(size)])


def exchanged(blocks, axes):
    return lax.all_to_all(blocks, axes, 0, 0, tiled=True)


def copies(value, count):
    return jnp.broadcast_to(value[None], (count, *value.shape))


def span_rows(first, second, shape):
    lane = lax.broadcasted_iota(jnp.int32, shape, 1)
    row = jnp.where(lane == 0, first, jnp.where(lane == 1, second, 0))
    return row.astype(jnp.float32).astype(jnp.bfloat16)


def project_kernel(zh_ref, span_ref, act_ref, w_ref, out_ref):
    zh = zh_ref[0]
    places, tokens = act_ref.shape[1:3]
    total = None
    for place in range(places):
        source = lax.rem(zh + place, places)
        for core in range(2):
            act = act_ref[core, place]
            w = w_ref[:, source * 2 + core]
            part = jnp.dot(act, w.reshape(-1, w.shape[-1]), preferred_element_type=jnp.float32)
            total = part if total is None else total + part
    rounded = total.astype(out_ref.dtype)
    spans = span_rows(span_ref[0], span_ref[1], (SPAN_ROWS, total.shape[1]))
    for peer in range(out_ref.shape[0]):
        out_ref[peer, :tokens, :] = rounded
        out_ref[peer, tokens:, :] = spans


def attend_kernel(q_ref, kv_ref, out_ref, stat_ref, pos_ref, *, scale):
    blocks, _, width = q_ref.shape
    chunks, peers = kv_ref.shape[:2]
    tokens = kv_ref.shape[2] - SPAN_ROWS
    rows = q_ref.shape[1] - SPAN_ROWS
    half = tokens // 2
    count = peers * tokens
    factor = scale * math.log2(math.e)

    lane = lax.broadcasted_iota(jnp.int32, (peers, count), 1)
    start = lax.broadcasted_iota(jnp.int32, (peers, count), 0) * tokens
    inside = lane - start
    early = (inside >= 0) & (inside < half)
    late = (inside >= half) & (inside < tokens)
    for chunk in range(chunks):
        held = kv_ref[chunk, :, tokens:, :128].astype(jnp.float32)
        spans = jnp.max(held, axis=1) * half
        place = jnp.where(early, spans[:, 0:1], jnp.where(late, spans[:, 1:2] - half, 0.0))
        place = place + jnp.where(early | late, inside.astype(jnp.float32), 0.0)
        pos_ref[chunk : chunk + 1, :] = jnp.sum(place, axis=0, keepdims=True)

    row = lax.broadcasted_iota(jnp.int32, (tokens, 1), 0).astype(jnp.float32)
    column = lax.broadcasted_iota(jnp.int32, (rows, 128), 1)
    stat_ref[...] = jnp.zeros(stat_ref.shape, jnp.float32)

    def step(block, carry):
        spans = q_ref[block, rows : rows + SPAN_ROWS, :].astype(jnp.float32) * half
        query_pos = jnp.where(row < half, spans[0:1, 0:1], spans[0:1, 1:2] - half) + row
        query_pos = jnp.concatenate([query_pos] * (rows // tokens), axis=0)
        query = q_ref[block, :rows, :]
        scores = []
        top = jnp.full((rows, 1), FLOOR, jnp.float32)
        for chunk in range(chunks):
            keys = kv_ref[chunk, :, :tokens, :width].reshape(count, width)
            score = lax.dot_general(
                query, keys, (((1,), (1,)), ((), ())), preferred_element_type=jnp.float32
            )
            score = jnp.where(pos_ref[chunk : chunk + 1, :] <= query_pos, score, HIDDEN)
            top = jnp.maximum(top, jnp.max(score, axis=1, keepdims=True))
            scores.append(score)
        total = jnp.zeros((rows, 1), jnp.float32)
        mixed = jnp.zeros((rows, width), jnp.float32)
        for chunk in range(chunks):
            values = kv_ref[chunk, :, :tokens, width:].reshape(count, width)
            weight = jnp.exp2((scores[chunk] - top) * factor)
            total = total + jnp.sum(weight, axis=1, keepdims=True)
            mixed = mixed + jnp.dot(
                weight.astype(jnp.bfloat16), values, preferred_element_type=jnp.float32
            )
        seen = total > 0.0
        safe = jnp.where(seen, total, 1.0)
        out_ref[block, :rows, :] = (mixed / safe).astype(jnp.bfloat16)
        size = jnp.where(seen, top * factor + jnp.log2(safe), HIDDEN)
        stat_ref[:rows, :] = jnp.where(column == block, size, stat_ref[:rows, :])
        return carry

    lax.fori_loop(0, blocks, step, 0)
    parts = []
    for chunk in range(stat_ref.shape[0] // 128):
        rest = stat_ref[chunk * 128 : (chunk + 1) * 128, :].T[:8]
        for third in range(3):
            high = rest.astype(jnp.bfloat16).astype(jnp.float32)
            parts.append((third * 4 + chunk, high))
            rest = rest - high
    place = lax.broadcasted_iota(jnp.int32, (STAT_ROWS, 128), 0)
    for block in range(blocks):
        tile = jnp.zeros((STAT_ROWS, 128), jnp.float32)
        for where, part in parts:
            tile = jnp.where(place == where, part[block : block + 1], tile)
        out_ref[block, rows:, :] = tile.astype(jnp.bfloat16)


def combine_kernel(in_ref, out_ref, total_ref, *, rows):
    blocks, _, width = in_ref.shape
    tokens = out_ref.shape[0]
    sizes = []
    for block in range(blocks):
        tile = in_ref[block, rows:, :].astype(jnp.float32)
        first = tile[:8]
        sizes.append(first + pltpu.roll(first, 4, 0) + tile[8:])
    top = sizes[0]
    for size in sizes[1:]:
        top = jnp.maximum(top, size)
    shares = [jnp.exp2(size - top) for size in sizes]
    whole = shares[0]
    for share in shares[1:]:
        whole = whole + share
    turned = jnp.concatenate([share / whole for share in shares], axis=0).T
    for start in range(0, rows, 128):
        count = min(128, rows - start)
        held = jnp.zeros((count, width), jnp.float32)
        for block in range(blocks):
            place = block * 8 + start // 128
            mixed = in_ref[block, start : start + count, :].astype(jnp.float32)
            held = held + turned[:count, place : place + 1] * mixed
        total_ref[start : start + count, :] = held
    for head in range(rows // tokens):
        kept = total_ref[head * tokens : (head + 1) * tokens, :]
        out_ref[:, head * width : (head + 1) * width] = kept.astype(out_ref.dtype)


VMEM = pl.BlockSpec(memory_space=pltpu.VMEM)
SMEM = pl.BlockSpec(memory_space=pltpu.SMEM)


def body(activations, queries, w_kv, span_of):
    tokens, features = activations.shape
    group, width = queries.shape[1:]
    rows = tokens * group
    ranks = lax.axis_size(HEADS)
    line = lax.axis_size("zl")
    plane = lax.axis_size(PLANE)
    side = lax.axis_size("y")
    zh = lax.axis_index("zh").astype(jnp.int32).reshape(1)

    left = shifted(activations, "zh", 1)
    right = shifted(activations, "zh", -1)
    cut = features // 2
    far_a = shifted(left[:, :cut], "zh", 1)
    far_b = shifted(right[:, cut:], "zh", -1)
    far = jnp.concatenate([far_a, far_b], axis=1)
    near = jnp.stack([activations, right, far, left])
    acts = lax.all_gather(near, "core")

    piece = w_kv.shape[0]
    w = w_kv.reshape(piece, ranks, 2 * width).transpose(1, 0, 2)
    w = exchanged(w, HEADS)
    w = exchanged(copies(w, line), "zl")
    w = w.transpose(1, 0, 2, 3).reshape(ranks, line * piece, 2 * width)
    w = exchanged(copies(w, plane), PLANE)

    spans = jnp.pad(span_of.astype(jnp.bfloat16)[None], ((0, SPAN_ROWS - 1), (0, width - 2)))
    q = queries.transpose(1, 0, 2).reshape(rows, width)
    q = exchanged(copies(jnp.concatenate([q, spans]), side), "y")

    kv = pl.pallas_call(
        project_kernel,
        out_shape=jax.ShapeDtypeStruct((line, tokens + SPAN_ROWS, 2 * width), jnp.bfloat16),
        in_specs=[SMEM, SMEM, VMEM, VMEM],
        out_specs=VMEM,
        name="project",
    )(zh, span_of, acts, w)
    kv = exchanged(kv, "zl")
    kv = exchanged(copies(kv, side), "x")

    padded = (rows + 127) // 128 * 128
    mixed = pl.pallas_call(
        lambda *refs: attend_kernel(*refs, scale=1.0 / math.sqrt(width)),
        out_shape=jax.ShapeDtypeStruct((side, rows + STAT_ROWS, width), jnp.bfloat16),
        in_specs=[VMEM, VMEM],
        out_specs=VMEM,
        scratch_shapes=[
            pltpu.VMEM((padded, 128), jnp.float32),
            pltpu.VMEM((8, line * tokens), jnp.float32),
        ],
        name="attend",
    )(q, kv)
    mixed = exchanged(mixed, "y")
    return pl.pallas_call(
        lambda *refs: combine_kernel(*refs, rows=rows),
        out_shape=jax.ShapeDtypeStruct((tokens, group * width), jnp.bfloat16),
        in_specs=[VMEM],
        out_specs=VMEM,
        scratch_shapes=[pltpu.VMEM((rows, width), jnp.float32)],
        name="combine",
    )(mixed)


def solution(mesh):
    finer = Mesh(mesh.devices.reshape(4, 2, 4, 4, 8), ("zh", "core", "x", "y", "zl"))
    in_specs = (P(ROWS, HEADS), P(ROWS, HEADS, None), P(HEADS + ROWS, None, None, None), P(ROWS))
    return jax.shard_map(body, mesh=finer, in_specs=in_specs, out_specs=P(ROWS, HEADS), check_vma=False)
```

```python
import math

import jax
import jax.numpy as jnp
from jax import lax
from jax.experimental import pallas as pl
from jax.experimental.pallas import tpu as pltpu
from jax.sharding import Mesh
from jax.sharding import PartitionSpec as P


ROWS = ("x", "y", "zl")
HEADS = ("zh", "core")
PLANE = ("x", "y")
HIDDEN = -1e30
FLOOR = -1e29
STAT_ROWS = 16
SPAN_ROWS = 8


def shifted(value, axis, by):
    size = lax.axis_size(axis)
    return lax.ppermute(value, axis, [(i, (i + by) % size) for i in range(size)])


def exchanged(blocks, axes):
    return lax.all_to_all(blocks, axes, 0, 0, tiled=True)


def copies(value, count):
    return jnp.broadcast_to(value[None], (count, *value.shape))


def span_rows(first, second, shape):
    lane = lax.broadcasted_iota(jnp.int32, shape, 1)
    row = jnp.where(lane == 0, first, jnp.where(lane == 1, second, 0))
    return row.astype(jnp.float32).astype(jnp.bfloat16)


def project_kernel(zh_ref, span_ref, act_ref, w_ref, out_ref):
    zh = zh_ref[0]
    places, tokens = act_ref.shape[1:3]
    total = None
    for place in range(places):
        source = lax.rem(zh + place, places)
        for core in range(2):
            act = act_ref[core, place]
            w = w_ref[:, source * 2 + core]
            part = jnp.dot(act, w.reshape(-1, w.shape[-1]), preferred_element_type=jnp.float32)
            total = part if total is None else total + part
    rounded = total.astype(out_ref.dtype)
    spans = span_rows(span_ref[0], span_ref[1], (SPAN_ROWS, total.shape[1]))
    for peer in range(out_ref.shape[0]):
        out_ref[peer, :tokens, :] = rounded
        out_ref[peer, tokens:, :] = spans


def attend_kernel(y_ref, q0_ref, q1_ref, q2_ref, q3_ref, kv_ref, out_ref, stat_ref, pos_ref, q_ref, *, scale):
    for place, source_ref in enumerate((q0_ref, q1_ref, q2_ref, q3_ref)):
        q_ref[place] = source_ref[...]
    own = y_ref[0]
    blocks, _, width = q_ref.shape
    chunks, peers = kv_ref.shape[:2]
    tokens = kv_ref.shape[2] - SPAN_ROWS
    rows = q_ref.shape[1] - SPAN_ROWS
    half = tokens // 2
    count = peers * tokens
    factor = scale * math.log2(math.e)

    lane = lax.broadcasted_iota(jnp.int32, (peers, count), 1)
    start = lax.broadcasted_iota(jnp.int32, (peers, count), 0) * tokens
    inside = lane - start
    early = (inside >= 0) & (inside < half)
    late = (inside >= half) & (inside < tokens)
    for chunk in range(chunks):
        held = kv_ref[chunk, :, tokens:, :128].astype(jnp.float32)
        spans = jnp.max(held, axis=1) * half
        place = jnp.where(early, spans[:, 0:1], jnp.where(late, spans[:, 1:2] - half, 0.0))
        place = place + jnp.where(early | late, inside.astype(jnp.float32), 0.0)
        pos_ref[chunk : chunk + 1, :] = jnp.sum(place, axis=0, keepdims=True)

    row = lax.broadcasted_iota(jnp.int32, (tokens, 1), 0).astype(jnp.float32)
    column = lax.broadcasted_iota(jnp.int32, (rows, 128), 1)
    stat_ref[...] = jnp.zeros(stat_ref.shape, jnp.float32)

    def step(block, carry):
        owner = lax.rem(own + blocks - block, blocks)
        spans = q_ref[block, rows : rows + SPAN_ROWS, :].astype(jnp.float32) * half
        query_pos = jnp.where(row < half, spans[0:1, 0:1], spans[0:1, 1:2] - half) + row
        query_pos = jnp.concatenate([query_pos] * (rows // tokens), axis=0)
        query = q_ref[block, :rows, :]
        scores = []
        top = jnp.full((rows, 1), FLOOR, jnp.float32)
        for chunk in range(chunks):
            keys = kv_ref[chunk, :, :tokens, :width].reshape(count, width)
            score = lax.dot_general(
                query, keys, (((1,), (1,)), ((), ())), preferred_element_type=jnp.float32
            )
            score = jnp.where(pos_ref[chunk : chunk + 1, :] <= query_pos, score, HIDDEN)
            top = jnp.maximum(top, jnp.max(score, axis=1, keepdims=True))
            scores.append(score)
        total = jnp.zeros((rows, 1), jnp.float32)
        mixed = jnp.zeros((rows, width), jnp.float32)
        for chunk in range(chunks):
            values = kv_ref[chunk, :, :tokens, width:].reshape(count, width)
            weight = jnp.exp2((scores[chunk] - top) * factor)
            total = total + jnp.sum(weight, axis=1, keepdims=True)
            mixed = mixed + jnp.dot(
                weight.astype(jnp.bfloat16), values, preferred_element_type=jnp.float32
            )
        seen = total > 0.0
        safe = jnp.where(seen, total, 1.0)
        out_ref[owner, :rows, :] = (mixed / safe).astype(jnp.bfloat16)
        size = jnp.where(seen, top * factor + jnp.log2(safe), HIDDEN)
        stat_ref[:rows, :] = jnp.where(column == owner, size, stat_ref[:rows, :])
        return carry

    lax.fori_loop(0, blocks, step, 0)
    parts = []
    for chunk in range(stat_ref.shape[0] // 128):
        rest = stat_ref[chunk * 128 : (chunk + 1) * 128, :].T[:8]
        for third in range(3):
            high = rest.astype(jnp.bfloat16).astype(jnp.float32)
            parts.append((third * 4 + chunk, high))
            rest = rest - high
    place = lax.broadcasted_iota(jnp.int32, (STAT_ROWS, 128), 0)
    for block in range(blocks):
        tile = jnp.zeros((STAT_ROWS, 128), jnp.float32)
        for where, part in parts:
            tile = jnp.where(place == where, part[block : block + 1], tile)
        out_ref[block, rows:, :] = tile.astype(jnp.bfloat16)


def combine_kernel(in_ref, out_ref, total_ref, *, rows):
    blocks, _, width = in_ref.shape
    tokens = out_ref.shape[0]
    sizes = []
    for block in range(blocks):
        tile = in_ref[block, rows:, :].astype(jnp.float32)
        first = tile[:8]
        sizes.append(first + pltpu.roll(first, 4, 0) + tile[8:])
    top = sizes[0]
    for size in sizes[1:]:
        top = jnp.maximum(top, size)
    shares = [jnp.exp2(size - top) for size in sizes]
    whole = shares[0]
    for share in shares[1:]:
        whole = whole + share
    turned = jnp.concatenate([share / whole for share in shares], axis=0).T
    for start in range(0, rows, 128):
        count = min(128, rows - start)
        held = jnp.zeros((count, width), jnp.float32)
        for block in range(blocks):
            place = block * 8 + start // 128
            mixed = in_ref[block, start : start + count, :].astype(jnp.float32)
            held = held + turned[:count, place : place + 1] * mixed
        total_ref[start : start + count, :] = held
    for head in range(rows // tokens):
        kept = total_ref[head * tokens : (head + 1) * tokens, :]
        out_ref[:, head * width : (head + 1) * width] = kept.astype(out_ref.dtype)


VMEM = pl.BlockSpec()
SMEM = pl.BlockSpec(memory_space=pltpu.SMEM)


def body(activations, queries, w_kv, span_of):
    tokens, features = activations.shape
    group, width = queries.shape[1:]
    rows = tokens * group
    ranks = lax.axis_size(HEADS)
    line = lax.axis_size("zl")
    plane = lax.axis_size(PLANE)
    side = lax.axis_size("y")
    zh = lax.axis_index("zh").astype(jnp.int32).reshape(1)
    own_y = lax.axis_index("y").astype(jnp.int32).reshape(1)

    left = shifted(activations, "zh", 1)
    right = shifted(activations, "zh", -1)
    cut = features // 2
    far_a = shifted(left[:, :cut], "zh", 1)
    far_b = shifted(right[:, cut:], "zh", -1)
    far = jnp.concatenate([far_a, far_b], axis=1)
    near = jnp.stack([activations, right, far, left])
    acts = lax.all_gather(near, "core")

    piece = w_kv.shape[0]
    w = w_kv.reshape(piece, ranks, 2 * width).transpose(1, 0, 2)
    w = exchanged(w, HEADS)
    w = exchanged(copies(w, line), "zl")
    w = w.transpose(1, 0, 2, 3).reshape(ranks, line * piece, 2 * width)
    w = exchanged(copies(w, plane), PLANE)

    spans = jnp.pad(span_of.astype(jnp.bfloat16)[None], ((0, SPAN_ROWS - 1), (0, width - 2)))
    q = queries.transpose(1, 0, 2).reshape(rows, width)
    q = jnp.concatenate([q, spans])
    moved = []
    for by in range(1, side):
        moved.append(shifted(q, "y", by))

    kv = pl.pallas_call(
        project_kernel,
        out_shape=jax.ShapeDtypeStruct((line, tokens + SPAN_ROWS, 2 * width), jnp.bfloat16),
        in_specs=[SMEM, SMEM, VMEM, VMEM],
        out_specs=VMEM,
        name="project",
        compiler_params=pltpu.CompilerParams(vmem_limit_bytes=12 * 1024 * 1024),
    )(zh, span_of, acts, w)
    kv = exchanged(kv, "zl")
    kv = exchanged(copies(kv, side), "x")

    padded = (rows + 127) // 128 * 128
    mixed = pl.pallas_call(
        lambda *refs: attend_kernel(*refs, scale=1.0 / math.sqrt(width)),
        out_shape=jax.ShapeDtypeStruct((side, rows + STAT_ROWS, width), jnp.bfloat16),
        in_specs=[SMEM] + [VMEM] * 5,
        out_specs=VMEM,
        scratch_shapes=[
            pltpu.VMEM((padded, 128), jnp.float32),
            pltpu.VMEM((8, line * tokens), jnp.float32),
            pltpu.VMEM((side, rows + SPAN_ROWS, width), jnp.bfloat16),
        ],
        name="attend",
        compiler_params=pltpu.CompilerParams(vmem_limit_bytes=20 * 1024 * 1024),
    )(own_y, q, *moved, kv)
    mixed = exchanged(mixed, "y")
    return pl.pallas_call(
        lambda *refs: combine_kernel(*refs, rows=rows),
        out_shape=jax.ShapeDtypeStruct((tokens, group * width), jnp.bfloat16),
        in_specs=[VMEM],
        out_specs=VMEM,
        scratch_shapes=[pltpu.VMEM((rows, width), jnp.float32)],
        name="combine",
        compiler_params=pltpu.CompilerParams(vmem_limit_bytes=8 * 1024 * 1024),
    )(mixed)


def solution(mesh):
    finer = Mesh(mesh.devices.reshape(4, 2, 4, 4, 8), ("zh", "core", "x", "y", "zl"))
    in_specs = (P(ROWS, HEADS), P(ROWS, HEADS, None), P(HEADS + ROWS, None, None, None), P(ROWS))
    return jax.shard_map(body, mesh=finer, in_specs=in_specs, out_specs=P(ROWS, HEADS), check_vma=False)
```

```python
import math

import jax
import jax.numpy as jnp
from jax import lax
from jax.experimental import pallas as pl
from jax.experimental.pallas import tpu as pltpu
from jax.sharding import Mesh
from jax.sharding import PartitionSpec as P


ROWS = ("x", "y", "zo", "zi")
HEADS = ("zh", "core")
PLANE = ("x", "y")
LINE = ("zo", "zi")
HIDDEN = -1e30
FLOOR = -1e29
STAT_ROWS = 16
SPAN_ROWS = 8


def shifted(value, axis, by):
    size = lax.axis_size(axis)
    return lax.ppermute(value, axis, [(i, (i + by) % size) for i in range(size)])


def exchanged(blocks, axes):
    return lax.all_to_all(blocks, axes, 0, 0, tiled=True)


def copies(value, count):
    return jnp.broadcast_to(value[None], (count, *value.shape))


def span_rows(first, second, shape):
    lane = lax.broadcasted_iota(jnp.int32, shape, 1)
    row = jnp.where(lane == 0, first, jnp.where(lane == 1, second, 0))
    return row.astype(jnp.float32).astype(jnp.bfloat16)


def project_kernel(zh_ref, span_ref, act_ref, w_ref, out_ref):
    zh = zh_ref[0]
    places, tokens = act_ref.shape[1:3]
    total = None
    for place in range(places):
        source = lax.rem(zh + place, places)
        for core in range(2):
            act = act_ref[core, place]
            w = w_ref[:, source * 2 + core]
            part = jnp.dot(act, w.reshape(-1, w.shape[-1]), preferred_element_type=jnp.float32)
            total = part if total is None else total + part
    rounded = total.astype(out_ref.dtype)
    out_ref[:tokens, :] = rounded
    out_ref[tokens:, :] = span_rows(span_ref[0], span_ref[1], (SPAN_ROWS, total.shape[1]))


def attend_kernel(own_ref, q0_ref, q1_ref, q2_ref, q3_ref, kv_ref, out_ref, stat_ref, pos_ref, q_ref, *, scale):
    for place, source_ref in enumerate((q0_ref, q1_ref, q2_ref, q3_ref)):
        q_ref[place] = source_ref[...]
    own = own_ref[0]
    blocks, _, width = q_ref.shape
    chunks, peers = kv_ref.shape[:2]
    tokens = kv_ref.shape[2] - SPAN_ROWS
    rows = q_ref.shape[1] - SPAN_ROWS
    half = tokens // 2
    count = peers * tokens
    factor = scale * math.log2(math.e)

    lane = lax.broadcasted_iota(jnp.int32, (peers, count), 1)
    start = lax.broadcasted_iota(jnp.int32, (peers, count), 0) * tokens
    inside = lane - start
    early = (inside >= 0) & (inside < half)
    late = (inside >= half) & (inside < tokens)
    for chunk in range(chunks):
        held = kv_ref[chunk, :, tokens:, :128].astype(jnp.float32)
        spans = jnp.max(held, axis=1) * half
        place = jnp.where(early, spans[:, 0:1], jnp.where(late, spans[:, 1:2] - half, 0.0))
        place = place + jnp.where(early | late, inside.astype(jnp.float32), 0.0)
        pos_ref[chunk : chunk + 1, :] = jnp.sum(place, axis=0, keepdims=True)

    row = lax.broadcasted_iota(jnp.int32, (tokens, 1), 0).astype(jnp.float32)
    column = lax.broadcasted_iota(jnp.int32, (rows, 128), 1)
    stat_ref[...] = jnp.zeros(stat_ref.shape, jnp.float32)

    def step(block, carry):
        owner = lax.rem(own + blocks - block, blocks)
        spans = q_ref[block, rows : rows + SPAN_ROWS, :].astype(jnp.float32) * half
        query_pos = jnp.where(row < half, spans[0:1, 0:1], spans[0:1, 1:2] - half) + row
        query_pos = jnp.concatenate([query_pos] * (rows // tokens), axis=0)
        query = q_ref[block, :rows, :]
        scores = []
        top = jnp.full((rows, 1), FLOOR, jnp.float32)
        for chunk in range(chunks):
            keys = kv_ref[chunk, :, :tokens, :width].reshape(count, width)
            score = lax.dot_general(
                query, keys, (((1,), (1,)), ((), ())), preferred_element_type=jnp.float32
            )
            score = jnp.where(pos_ref[chunk : chunk + 1, :] <= query_pos, score, HIDDEN)
            top = jnp.maximum(top, jnp.max(score, axis=1, keepdims=True))
            scores.append(score)
        total = jnp.zeros((rows, 1), jnp.float32)
        mixed = jnp.zeros((rows, width), jnp.float32)
        for chunk in range(chunks):
            values = kv_ref[chunk, :, :tokens, width:].reshape(count, width)
            weight = jnp.exp2((scores[chunk] - top) * factor)
            total = total + jnp.sum(weight, axis=1, keepdims=True)
            mixed = mixed + jnp.dot(
                weight.astype(jnp.bfloat16), values, preferred_element_type=jnp.float32
            )
        seen = total > 0.0
        safe = jnp.where(seen, total, 1.0)
        out_ref[owner, :rows, :] = (mixed / safe).astype(jnp.bfloat16)
        size = jnp.where(seen, top * factor + jnp.log2(safe), HIDDEN)
        stat_ref[:rows, :] = jnp.where(column == owner, size, stat_ref[:rows, :])
        return carry

    lax.fori_loop(0, blocks, step, 0)
    parts = []
    for chunk in range(stat_ref.shape[0] // 128):
        rest = stat_ref[chunk * 128 : (chunk + 1) * 128, :].T[:8]
        for third in range(3):
            high = rest.astype(jnp.bfloat16).astype(jnp.float32)
            parts.append((third * 4 + chunk, high))
            rest = rest - high
    place = lax.broadcasted_iota(jnp.int32, (STAT_ROWS, 128), 0)
    for block in range(blocks):
        tile = jnp.zeros((STAT_ROWS, 128), jnp.float32)
        for where, part in parts:
            tile = jnp.where(place == where, part[block : block + 1], tile)
        out_ref[block, rows:, :] = tile.astype(jnp.bfloat16)


def combine_kernel(in_ref, out_ref, total_ref, *, rows):
    blocks, _, width = in_ref.shape
    tokens = out_ref.shape[0]
    sizes = []
    for block in range(blocks):
        tile = in_ref[block, rows:, :].astype(jnp.float32)
        first = tile[:8]
        sizes.append(first + pltpu.roll(first, 4, 0) + tile[8:])
    top = sizes[0]
    for size in sizes[1:]:
        top = jnp.maximum(top, size)
    shares = [jnp.exp2(size - top) for size in sizes]
    whole = shares[0]
    for share in shares[1:]:
        whole = whole + share
    turned = jnp.concatenate([share / whole for share in shares], axis=0).T
    for start in range(0, rows, 128):
        count = min(128, rows - start)
        held = jnp.zeros((count, width), jnp.float32)
        for block in range(blocks):
            place = block * 8 + start // 128
            mixed = in_ref[block, start : start + count, :].astype(jnp.float32)
            held = held + turned[:count, place : place + 1] * mixed
        total_ref[start : start + count, :] = held
    for head in range(rows // tokens):
        kept = total_ref[head * tokens : (head + 1) * tokens, :]
        out_ref[:, head * width : (head + 1) * width] = kept.astype(out_ref.dtype)


VMEM = pl.BlockSpec()
SMEM = pl.BlockSpec(memory_space=pltpu.SMEM)


def body(activations, queries, w_kv, span_of):
    tokens, _ = activations.shape
    group, width = queries.shape[1:]
    rows = tokens * group
    ranks = lax.axis_size(HEADS)
    line = lax.axis_size(LINE)
    plane = lax.axis_size(PLANE)
    side = lax.axis_size("zi")
    zh = lax.axis_index("zh").astype(jnp.int32).reshape(1)
    own = lax.axis_index("zi").astype(jnp.int32).reshape(1)

    left = shifted(activations, "zh", 1)
    right = shifted(activations, "zh", -1)
    far = shifted(activations, "zh", 2)
    near = jnp.stack([activations, right, far, left])
    acts = lax.all_gather(near, "core")

    piece = w_kv.shape[0]
    w = w_kv.reshape(piece, ranks, 2 * width).transpose(1, 0, 2)
    w = exchanged(w, HEADS)
    w = exchanged(copies(w, line), LINE)
    w = w.transpose(1, 0, 2, 3).reshape(ranks, line * piece, 2 * width)
    w = exchanged(copies(w, plane), PLANE)

    spans = jnp.pad(span_of.astype(jnp.bfloat16)[None], ((0, SPAN_ROWS - 1), (0, width - 2)))
    q = queries.transpose(1, 0, 2).reshape(rows, width)
    q = jnp.concatenate([q, spans])
    moved = []
    for by in range(1, side):
        moved.append(shifted(q, "zi", by))

    kv = pl.pallas_call(
        project_kernel,
        out_shape=jax.ShapeDtypeStruct((tokens + SPAN_ROWS, 2 * width), jnp.bfloat16),
        in_specs=[SMEM, SMEM, VMEM, VMEM],
        out_specs=VMEM,
        name="project",
        compiler_params=pltpu.CompilerParams(vmem_limit_bytes=12 * 1024 * 1024),
    )(zh, span_of, acts, w)
    kv = jnp.stack([kv, shifted(kv, "zo", 1)])
    kv = exchanged(copies(kv, plane), PLANE)
    kv = kv.reshape(side, plane * 2 // side, tokens + SPAN_ROWS, 2 * width)

    padded = (rows + 127) // 128 * 128
    mixed = pl.pallas_call(
        lambda *refs: attend_kernel(*refs, scale=1.0 / math.sqrt(width)),
        out_shape=jax.ShapeDtypeStruct((side, rows + STAT_ROWS, width), jnp.bfloat16),
        in_specs=[SMEM] + [VMEM] * 5,
        out_specs=VMEM,
        scratch_shapes=[
            pltpu.VMEM((padded, 128), jnp.float32),
            pltpu.VMEM((8, plane * 2 // side * tokens), jnp.float32),
            pltpu.VMEM((side, rows + SPAN_ROWS, width), jnp.bfloat16),
        ],
        name="attend",
        compiler_params=pltpu.CompilerParams(vmem_limit_bytes=20 * 1024 * 1024),
    )(own, q, *moved, kv)
    mixed = exchanged(mixed, "zi")
    return pl.pallas_call(
        lambda *refs: combine_kernel(*refs, rows=rows),
        out_shape=jax.ShapeDtypeStruct((tokens, group * width), jnp.bfloat16),
        in_specs=[VMEM],
        out_specs=VMEM,
        scratch_shapes=[pltpu.VMEM((rows, width), jnp.float32)],
        name="combine",
        compiler_params=pltpu.CompilerParams(vmem_limit_bytes=8 * 1024 * 1024),
    )(mixed)


def solution(mesh):
    finer = Mesh(mesh.devices.reshape(4, 2, 4, 4, 2, 4), ("zh", "core", "x", "y", "zo", "zi"))
    in_specs = (P(ROWS, HEADS), P(ROWS, HEADS, None), P(HEADS + ROWS, None, None, None), P(ROWS))
    return jax.shard_map(body, mesh=finer, in_specs=in_specs, out_specs=P(ROWS, HEADS), check_vma=False)
```

```python
import math

import jax
import jax.numpy as jnp
from jax import lax
from jax.experimental import pallas as pl
from jax.experimental.pallas import tpu as pltpu
from jax.sharding import Mesh
from jax.sharding import PartitionSpec as P


ROWS = ("x", "y", "zo", "zi")
HEADS = ("zh", "core")
PLANE = ("x", "y")
LINE = ("zo", "zi")
HIDDEN = -1e30
FLOOR = -1e29
STAT_ROWS = 16
SPAN_ROWS = 8


def shifted(value, axis, by):
    size = lax.axis_size(axis)
    return lax.ppermute(value, axis, [(i, (i + by) % size) for i in range(size)])


def exchanged(blocks, axes):
    return lax.all_to_all(blocks, axes, 0, 0, tiled=True)


def copies(value, count):
    return jnp.broadcast_to(value[None], (count, *value.shape))


def span_rows(first, second, shape):
    lane = lax.broadcasted_iota(jnp.int32, shape, 1)
    row = jnp.where(lane == 0, first, jnp.where(lane == 1, second, 0))
    return row.astype(jnp.float32).astype(jnp.bfloat16)


def project_kernel(zh_ref, span_ref, chip_ref, others_ref, w_ref, out_ref):
    zh = zh_ref[0]
    tokens = chip_ref.shape[1]
    places = w_ref.shape[1] // 2
    total = None
    for core in range(2):
        near = [chip_ref[core], others_ref[1, core], others_ref[core, 2], others_ref[0, core]]
        for place, act in enumerate(near):
            source = lax.rem(zh + place, places)
            w = w_ref[:, source * 2 + core]
            part = jnp.dot(act, w.reshape(-1, w.shape[-1]), preferred_element_type=jnp.float32)
            total = part if total is None else total + part
    rounded = total.astype(out_ref.dtype)
    out_ref[:tokens, :] = rounded
    out_ref[tokens:, :] = span_rows(span_ref[0], span_ref[1], (SPAN_ROWS, total.shape[1]))


def attend_kernel(own_ref, q0_ref, q1_ref, q2_ref, q3_ref, kv_ref, out_ref, stat_ref, pos_ref, q_ref, *, scale):
    for place, source_ref in enumerate((q0_ref, q1_ref, q2_ref, q3_ref)):
        q_ref[place] = source_ref[...]
    own = own_ref[0]
    blocks, _, width = q_ref.shape
    chunks, peers = kv_ref.shape[:2]
    tokens = kv_ref.shape[2] - SPAN_ROWS
    rows = q_ref.shape[1] - SPAN_ROWS
    half = tokens // 2
    count = peers * tokens
    factor = scale * math.log2(math.e)

    lane = lax.broadcasted_iota(jnp.int32, (peers, count), 1)
    start = lax.broadcasted_iota(jnp.int32, (peers, count), 0) * tokens
    inside = lane - start
    early = (inside >= 0) & (inside < half)
    late = (inside >= half) & (inside < tokens)
    for chunk in range(chunks):
        held = kv_ref[chunk, :, tokens:, :128].astype(jnp.float32)
        spans = jnp.max(held, axis=1) * half
        place = jnp.where(early, spans[:, 0:1], jnp.where(late, spans[:, 1:2] - half, 0.0))
        place = place + jnp.where(early | late, inside.astype(jnp.float32), 0.0)
        pos_ref[chunk : chunk + 1, :] = jnp.sum(place, axis=0, keepdims=True)

    row = lax.broadcasted_iota(jnp.int32, (tokens, 1), 0).astype(jnp.float32)
    column = lax.broadcasted_iota(jnp.int32, (rows, 128), 1)
    stat_ref[...] = jnp.zeros(stat_ref.shape, jnp.float32)

    def step(block, carry):
        owner = lax.rem(own + blocks - block, blocks)
        spans = q_ref[block, rows : rows + SPAN_ROWS, :].astype(jnp.float32) * half
        query_pos = jnp.where(row < half, spans[0:1, 0:1], spans[0:1, 1:2] - half) + row
        query_pos = jnp.concatenate([query_pos] * (rows // tokens), axis=0)
        query = q_ref[block, :rows, :]
        scores = []
        top = jnp.full((rows, 1), FLOOR, jnp.float32)
        for chunk in range(chunks):
            keys = kv_ref[chunk, :, :tokens, :width].reshape(count, width)
            score = lax.dot_general(
                query, keys, (((1,), (1,)), ((), ())), preferred_element_type=jnp.float32
            )
            score = jnp.where(pos_ref[chunk : chunk + 1, :] <= query_pos, score, HIDDEN)
            top = jnp.maximum(top, jnp.max(score, axis=1, keepdims=True))
            scores.append(score)
        total = jnp.zeros((rows, 1), jnp.float32)
        mixed = jnp.zeros((rows, width), jnp.float32)
        for chunk in range(chunks):
            values = kv_ref[chunk, :, :tokens, width:].reshape(count, width)
            weight = jnp.exp2((scores[chunk] - top) * factor)
            total = total + jnp.sum(weight, axis=1, keepdims=True)
            mixed = mixed + jnp.dot(
                weight.astype(jnp.bfloat16), values, preferred_element_type=jnp.float32
            )
        seen = total > 0.0
        safe = jnp.where(seen, total, 1.0)
        out_ref[owner, :rows, :] = (mixed / safe).astype(jnp.bfloat16)
        size = jnp.where(seen, top * factor + jnp.log2(safe), HIDDEN)
        stat_ref[:rows, :] = jnp.where(column == owner, size, stat_ref[:rows, :])
        return carry

    lax.fori_loop(0, blocks, step, 0)
    parts = []
    for chunk in range(stat_ref.shape[0] // 128):
        rest = stat_ref[chunk * 128 : (chunk + 1) * 128, :].T[:8]
        for third in range(3):
            high = rest.astype(jnp.bfloat16).astype(jnp.float32)
            parts.append((third * 4 + chunk, high))
            rest = rest - high
    place = lax.broadcasted_iota(jnp.int32, (STAT_ROWS, 128), 0)
    for block in range(blocks):
        tile = jnp.zeros((STAT_ROWS, 128), jnp.float32)
        for where, part in parts:
            tile = jnp.where(place == where, part[block : block + 1], tile)
        out_ref[block, rows:, :] = tile.astype(jnp.bfloat16)


def combine_kernel(in_ref, out_ref, total_ref, *, rows):
    blocks, _, width = in_ref.shape
    tokens = out_ref.shape[0]
    sizes = []
    for block in range(blocks):
        tile = in_ref[block, rows:, :].astype(jnp.float32)
        first = tile[:8]
        sizes.append(first + pltpu.roll(first, 4, 0) + tile[8:])
    top = sizes[0]
    for size in sizes[1:]:
        top = jnp.maximum(top, size)
    shares = [jnp.exp2(size - top) for size in sizes]
    whole = shares[0]
    for share in shares[1:]:
        whole = whole + share
    turned = jnp.concatenate([share / whole for share in shares], axis=0).T
    for start in range(0, rows, 128):
        count = min(128, rows - start)
        held = jnp.zeros((count, width), jnp.float32)
        for block in range(blocks):
            place = block * 8 + start // 128
            mixed = in_ref[block, start : start + count, :].astype(jnp.float32)
            held = held + turned[:count, place : place + 1] * mixed
        total_ref[start : start + count, :] = held
    for head in range(rows // tokens):
        kept = total_ref[head * tokens : (head + 1) * tokens, :]
        out_ref[:, head * width : (head + 1) * width] = kept.astype(out_ref.dtype)


VMEM = pl.BlockSpec()
SMEM = pl.BlockSpec(memory_space=pltpu.SMEM)


def body(activations, queries, w_kv, span_of):
    tokens, _ = activations.shape
    group, width = queries.shape[1:]
    rows = tokens * group
    ranks = lax.axis_size(HEADS)
    line = lax.axis_size(LINE)
    plane = lax.axis_size(PLANE)
    side = lax.axis_size("zi")
    zh = lax.axis_index("zh").astype(jnp.int32).reshape(1)
    own = lax.axis_index("zi").astype(jnp.int32).reshape(1)

    slabs = lax.axis_size("zh")
    turn = [(2 * i + c, 2 * ((i + 1 - 2 * c) % slabs) + c) for i in range(slabs) for c in range(2)]
    chip = lax.all_gather(activations, "core")
    near = lax.ppermute(chip, HEADS, turn)
    far = shifted(activations, "zh", 2)
    others = lax.all_gather(jnp.concatenate([near, far[None]]), "core")

    piece = w_kv.shape[0]
    w = w_kv.reshape(piece, ranks, 2 * width).transpose(1, 0, 2)
    w = exchanged(w, HEADS)
    w = exchanged(copies(w, line), LINE)
    w = w.transpose(1, 0, 2, 3).reshape(ranks, line * piece, 2 * width)
    w = exchanged(copies(w, plane), PLANE)

    spans = jnp.pad(span_of.astype(jnp.bfloat16)[None], ((0, SPAN_ROWS - 1), (0, width - 2)))
    q = queries.transpose(1, 0, 2).reshape(rows, width)
    q = jnp.concatenate([q, spans])
    moved = []
    for by in range(1, side):
        moved.append(shifted(q, "zi", by))

    kv = pl.pallas_call(
        project_kernel,
        out_shape=jax.ShapeDtypeStruct((tokens + SPAN_ROWS, 2 * width), jnp.bfloat16),
        in_specs=[SMEM, SMEM, VMEM, VMEM, VMEM],
        out_specs=VMEM,
        name="project",
        compiler_params=pltpu.CompilerParams(vmem_limit_bytes=12 * 1024 * 1024),
    )(zh, span_of, chip, others, w)
    kv = jnp.stack([kv, shifted(kv, "zo", 1)])
    kv = exchanged(copies(kv, plane), PLANE)
    kv = kv.reshape(side, plane * 2 // side, tokens + SPAN_ROWS, 2 * width)

    padded = (rows + 127) // 128 * 128
    mixed = pl.pallas_call(
        lambda *refs: attend_kernel(*refs, scale=1.0 / math.sqrt(width)),
        out_shape=jax.ShapeDtypeStruct((side, rows + STAT_ROWS, width), jnp.bfloat16),
        in_specs=[SMEM] + [VMEM] * 5,
        out_specs=VMEM,
        scratch_shapes=[
            pltpu.VMEM((padded, 128), jnp.float32),
            pltpu.VMEM((8, plane * 2 // side * tokens), jnp.float32),
            pltpu.VMEM((side, rows + SPAN_ROWS, width), jnp.bfloat16),
        ],
        name="attend",
        compiler_params=pltpu.CompilerParams(vmem_limit_bytes=20 * 1024 * 1024),
    )(own, q, *moved, kv)
    mixed = exchanged(mixed, "zi")
    return pl.pallas_call(
        lambda *refs: combine_kernel(*refs, rows=rows),
        out_shape=jax.ShapeDtypeStruct((tokens, group * width), jnp.bfloat16),
        in_specs=[VMEM],
        out_specs=VMEM,
        scratch_shapes=[pltpu.VMEM((rows, width), jnp.float32)],
        name="combine",
        compiler_params=pltpu.CompilerParams(vmem_limit_bytes=8 * 1024 * 1024),
    )(mixed)


def solution(mesh):
    finer = Mesh(mesh.devices.reshape(4, 2, 4, 4, 2, 4), ("zh", "core", "x", "y", "zo", "zi"))
    in_specs = (P(ROWS, HEADS), P(ROWS, HEADS, None), P(HEADS + ROWS, None, None, None), P(ROWS))
    return jax.shard_map(body, mesh=finer, in_specs=in_specs, out_specs=P(ROWS, HEADS), check_vma=False)
```

```python
import math

import jax
import jax.numpy as jnp
from jax import lax
from jax.experimental import pallas as pl
from jax.experimental.pallas import tpu as pltpu
from jax.sharding import Mesh
from jax.sharding import PartitionSpec as P


ROWS = ("x", "y", "zo", "zi")
HEADS = ("zh", "core")
PLANE = ("x", "y")
LINE = ("zo", "zi")
HIDDEN = -1e30
FLOOR = -1e29
STAT_ROWS = 16
SPAN_ROWS = 8


def shifted(value, axis, by):
    size = lax.axis_size(axis)
    return lax.ppermute(value, axis, [(i, (i + by) % size) for i in range(size)])


def exchanged(blocks, axes):
    return lax.all_to_all(blocks, axes, 0, 0, tiled=True)


def copies(value, count):
    return jnp.broadcast_to(value[None], (count, *value.shape))


def span_rows(first, second, shape):
    lane = lax.broadcasted_iota(jnp.int32, shape, 1)
    row = jnp.where(lane == 0, first, jnp.where(lane == 1, second, 0))
    return row.astype(jnp.float32).astype(jnp.bfloat16)


def project_kernel(zh_ref, span_ref, chip_ref, others_ref, w_ref, out_ref):
    zh = zh_ref[0]
    tokens = chip_ref.shape[1]
    places = w_ref.shape[1] // 2
    total = None
    for core in range(2):
        near = [chip_ref[core], others_ref[1, core], others_ref[core, 2], others_ref[0, core]]
        for place, act in enumerate(near):
            source = lax.rem(zh + place, places)
            w = w_ref[:, source * 2 + core]
            part = jnp.dot(act, w.reshape(-1, w.shape[-1]), preferred_element_type=jnp.float32)
            total = part if total is None else total + part
    rounded = total.astype(out_ref.dtype)
    out_ref[:tokens, :] = rounded
    out_ref[tokens:, :] = span_rows(span_ref[0], span_ref[1], (SPAN_ROWS, total.shape[1]))


def column_of(table, lane, place):
    return jnp.sum(jnp.where(lane == place, table, 0.0), axis=1, keepdims=True)


def attend_block(query, query_pos, kv_ref, pos_ref, top, total, mixed, factor):
    chunks, peers = kv_ref.shape[:2]
    width = query.shape[1]
    tokens = kv_ref.shape[2] - SPAN_ROWS
    count = peers * tokens
    scores = []
    first = top
    for chunk in range(chunks):
        keys = kv_ref[chunk, :, :tokens, :width].reshape(count, width)
        score = lax.dot_general(
            query, keys, (((1,), (1,)), ((), ())), preferred_element_type=jnp.float32
        )
        score = jnp.where(pos_ref[chunk : chunk + 1, :] <= query_pos, score, HIDDEN)
        top = jnp.maximum(top, jnp.max(score, axis=1, keepdims=True))
        scores.append(score)
    if total is None:
        total = jnp.zeros(top.shape, jnp.float32)
        mixed = jnp.zeros(query.shape, jnp.float32)
    else:
        kept = jnp.exp2((first - top) * factor)
        total = total * kept
        mixed = mixed * kept
    for chunk in range(chunks):
        values = kv_ref[chunk, :, :tokens, width:].reshape(count, width)
        weight = jnp.exp2((scores[chunk] - top) * factor)
        total = total + jnp.sum(weight, axis=1, keepdims=True)
        mixed = mixed + jnp.dot(
            weight.astype(jnp.bfloat16), values, preferred_element_type=jnp.float32
        )
    return top, total, mixed


def fill_positions(kv_ref, pos_ref):
    chunks, peers = kv_ref.shape[:2]
    tokens = kv_ref.shape[2] - SPAN_ROWS
    half = tokens // 2
    count = peers * tokens
    lane = lax.broadcasted_iota(jnp.int32, (peers, count), 1)
    inside = lane - lax.broadcasted_iota(jnp.int32, (peers, count), 0) * tokens
    early = (inside >= 0) & (inside < half)
    late = (inside >= half) & (inside < tokens)
    for chunk in range(chunks):
        held = kv_ref[chunk, :, tokens:, :128].astype(jnp.float32)
        spans = jnp.max(held, axis=1) * half
        place = jnp.where(early, spans[:, 0:1], jnp.where(late, spans[:, 1:2] - half, 0.0))
        place = place + jnp.where(early | late, inside.astype(jnp.float32), 0.0)
        pos_ref[chunk : chunk + 1, :] = jnp.sum(place, axis=0, keepdims=True)


def query_positions(q_ref, block, rows, tokens):
    half = tokens // 2
    row = lax.broadcasted_iota(jnp.int32, (tokens, 1), 0).astype(jnp.float32)
    spans = q_ref[block, rows : rows + SPAN_ROWS, :].astype(jnp.float32) * half
    query_pos = jnp.where(row < half, spans[0:1, 0:1], spans[0:1, 1:2] - half) + row
    return jnp.concatenate([query_pos] * (rows // tokens), axis=0)


def begin_kernel(q0_ref, q1_ref, q2_ref, q3_ref, kv_ref, mixed_ref, state_ref, pos_ref, q_ref, *, scale):
    for place, source_ref in enumerate((q0_ref, q1_ref, q2_ref, q3_ref)):
        q_ref[place] = source_ref[...]
    blocks = q_ref.shape[0]
    rows = q_ref.shape[1] - SPAN_ROWS
    factor = scale * math.log2(math.e)
    fill_positions(kv_ref, pos_ref)
    lane = lax.broadcasted_iota(jnp.int32, (rows, 128), 1)
    state_ref[...] = jnp.zeros(state_ref.shape, jnp.float32)

    def step(block, carry):
        query_pos = query_positions(q_ref, block, rows, kv_ref.shape[2] - SPAN_ROWS)
        top = jnp.full((rows, 1), FLOOR, jnp.float32)
        query = q_ref[block, :rows, :]
        top, total, mixed = attend_block(query, query_pos, kv_ref, pos_ref, top, None, None, factor)
        mixed_ref[block] = mixed
        state = jnp.where(lane == block, top, state_ref[...])
        state_ref[...] = jnp.where(lane == block + 8, total, state)
        return carry

    lax.fori_loop(0, blocks, step, 0)


def finish_kernel(
    own_ref, q0_ref, q1_ref, q2_ref, q3_ref, kv_ref, mixed_ref, state_ref,
    out_ref, stat_ref, pos_ref, q_ref, *, scale
):
    for place, source_ref in enumerate((q0_ref, q1_ref, q2_ref, q3_ref)):
        q_ref[place] = source_ref[...]
    own = own_ref[0]
    blocks = q_ref.shape[0]
    rows = q_ref.shape[1] - SPAN_ROWS
    factor = scale * math.log2(math.e)
    fill_positions(kv_ref, pos_ref)
    lane = lax.broadcasted_iota(jnp.int32, (rows, 128), 1)
    stat_ref[...] = jnp.zeros(stat_ref.shape, jnp.float32)

    def step(block, carry):
        owner = lax.rem(own + blocks - block, blocks)
        query_pos = query_positions(q_ref, block, rows, kv_ref.shape[2] - SPAN_ROWS)
        state = state_ref[...]
        top = column_of(state, lane, block)
        total = column_of(state, lane, block + 8)
        query = q_ref[block, :rows, :]
        top, total, mixed = attend_block(
            query, query_pos, kv_ref, pos_ref, top, total, mixed_ref[block], factor
        )
        seen = total > 0.0
        safe = jnp.where(seen, total, 1.0)
        out_ref[owner, :rows, :] = (mixed / safe).astype(jnp.bfloat16)
        size = jnp.where(seen, top * factor + jnp.log2(safe), HIDDEN)
        stat_ref[:rows, :] = jnp.where(lane == owner, size, stat_ref[:rows, :])
        return carry

    lax.fori_loop(0, blocks, step, 0)
    parts = []
    for chunk in range(stat_ref.shape[0] // 128):
        rest = stat_ref[chunk * 128 : (chunk + 1) * 128, :].T[:8]
        for third in range(3):
            high = rest.astype(jnp.bfloat16).astype(jnp.float32)
            parts.append((third * 4 + chunk, high))
            rest = rest - high
    place = lax.broadcasted_iota(jnp.int32, (STAT_ROWS, 128), 0)
    for block in range(blocks):
        tile = jnp.zeros((STAT_ROWS, 128), jnp.float32)
        for where, part in parts:
            tile = jnp.where(place == where, part[block : block + 1], tile)
        out_ref[block, rows:, :] = tile.astype(jnp.bfloat16)


def combine_kernel(in_ref, out_ref, total_ref, *, rows):
    blocks, _, width = in_ref.shape
    tokens = out_ref.shape[0]
    sizes = []
    for block in range(blocks):
        tile = in_ref[block, rows:, :].astype(jnp.float32)
        first = tile[:8]
        sizes.append(first + pltpu.roll(first, 4, 0) + tile[8:])
    top = sizes[0]
    for size in sizes[1:]:
        top = jnp.maximum(top, size)
    shares = [jnp.exp2(size - top) for size in sizes]
    whole = shares[0]
    for share in shares[1:]:
        whole = whole + share
    turned = jnp.concatenate([share / whole for share in shares], axis=0).T
    for start in range(0, rows, 128):
        count = min(128, rows - start)
        held = jnp.zeros((count, width), jnp.float32)
        for block in range(blocks):
            place = block * 8 + start // 128
            mixed = in_ref[block, start : start + count, :].astype(jnp.float32)
            held = held + turned[:count, place : place + 1] * mixed
        total_ref[start : start + count, :] = held
    for head in range(rows // tokens):
        kept = total_ref[head * tokens : (head + 1) * tokens, :]
        out_ref[:, head * width : (head + 1) * width] = kept.astype(out_ref.dtype)


VMEM = pl.BlockSpec()
SMEM = pl.BlockSpec(memory_space=pltpu.SMEM)


def body(activations, queries, w_kv, span_of):
    tokens, _ = activations.shape
    group, width = queries.shape[1:]
    rows = tokens * group
    ranks = lax.axis_size(HEADS)
    line = lax.axis_size(LINE)
    plane = lax.axis_size(PLANE)
    side = lax.axis_size("zi")
    zh = lax.axis_index("zh").astype(jnp.int32).reshape(1)
    own = lax.axis_index("zi").astype(jnp.int32).reshape(1)

    slabs = lax.axis_size("zh")
    turn = [(2 * i + c, 2 * ((i + 1 - 2 * c) % slabs) + c) for i in range(slabs) for c in range(2)]
    chip = lax.all_gather(activations, "core")
    near = lax.ppermute(chip, HEADS, turn)
    far = shifted(activations, "zh", 2)
    others = lax.all_gather(jnp.concatenate([near, far[None]]), "core")

    piece = w_kv.shape[0]
    w = w_kv.reshape(piece, ranks, 2 * width).transpose(1, 0, 2)
    w = exchanged(w, HEADS)
    w = exchanged(copies(w, line), LINE)
    w = w.transpose(1, 0, 2, 3).reshape(ranks, line * piece, 2 * width)
    w = exchanged(copies(w, plane), PLANE)

    spans = jnp.pad(span_of.astype(jnp.bfloat16)[None], ((0, SPAN_ROWS - 1), (0, width - 2)))
    q = queries.transpose(1, 0, 2).reshape(rows, width)
    q = jnp.concatenate([q, spans])
    moved = []
    for by in range(1, side):
        moved.append(shifted(q, "zi", by))

    kv = pl.pallas_call(
        project_kernel,
        out_shape=jax.ShapeDtypeStruct((tokens + SPAN_ROWS, 2 * width), jnp.bfloat16),
        in_specs=[SMEM, SMEM, VMEM, VMEM, VMEM],
        out_specs=VMEM,
        name="project",
        compiler_params=pltpu.CompilerParams(vmem_limit_bytes=12 * 1024 * 1024),
    )(zh, span_of, chip, others, w)
    sets = (2, plane // 2, tokens + SPAN_ROWS, 2 * width)
    other = shifted(kv, "zo", 1)
    first = exchanged(copies(kv, plane), PLANE).reshape(sets)
    spread = copies(other, plane)
    second = exchanged(spread, PLANE).reshape(sets)

    padded = (rows + 127) // 128 * 128
    scale = 1.0 / math.sqrt(width)
    positions = pltpu.VMEM((8, plane // 2 * tokens), jnp.float32)
    held = pltpu.VMEM((side, rows + SPAN_ROWS, width), jnp.bfloat16)
    mixed, state = pl.pallas_call(
        lambda *refs: begin_kernel(*refs, scale=scale),
        out_shape=(
            jax.ShapeDtypeStruct((side, rows, width), jnp.float32),
            jax.ShapeDtypeStruct((rows, 128), jnp.float32),
        ),
        in_specs=[VMEM] * 5,
        out_specs=(VMEM, VMEM),
        scratch_shapes=[positions, held],
        name="begin",
        compiler_params=pltpu.CompilerParams(vmem_limit_bytes=16 * 1024 * 1024),
    )(q, *moved, first)
    mixed = pl.pallas_call(
        lambda *refs: finish_kernel(*refs, scale=scale),
        out_shape=jax.ShapeDtypeStruct((side, rows + STAT_ROWS, width), jnp.bfloat16),
        in_specs=[SMEM] + [VMEM] * 7,
        out_specs=VMEM,
        scratch_shapes=[pltpu.VMEM((padded, 128), jnp.float32), positions, held],
        name="finish",
        compiler_params=pltpu.CompilerParams(vmem_limit_bytes=16 * 1024 * 1024),
    )(own, q, *moved, second, mixed, state)
    mixed = exchanged(mixed, "zi")
    return pl.pallas_call(
        lambda *refs: combine_kernel(*refs, rows=rows),
        out_shape=jax.ShapeDtypeStruct((tokens, group * width), jnp.bfloat16),
        in_specs=[VMEM],
        out_specs=VMEM,
        scratch_shapes=[pltpu.VMEM((rows, width), jnp.float32)],
        name="combine",
        compiler_params=pltpu.CompilerParams(vmem_limit_bytes=8 * 1024 * 1024),
    )(mixed)


def solution(mesh):
    finer = Mesh(mesh.devices.reshape(4, 2, 4, 4, 2, 4), ("zh", "core", "x", "y", "zo", "zi"))
    in_specs = (P(ROWS, HEADS), P(ROWS, HEADS, None), P(HEADS + ROWS, None, None, None), P(ROWS))
    return jax.shard_map(body, mesh=finer, in_specs=in_specs, out_specs=P(ROWS, HEADS), check_vma=False)
```

```python
import math

import jax
import jax.numpy as jnp
from jax import lax
from jax.experimental import pallas as pl
from jax.experimental.pallas import tpu as pltpu
from jax.sharding import Mesh
from jax.sharding import PartitionSpec as P


ROWS = ("x", "y", "zo", "zi")
HEADS = ("zh", "core")
PLANE = ("x", "y")
LINE = ("zo", "zi")
HIDDEN = -1e30
FLOOR = -1e29
STAT_ROWS = 16
SPAN_ROWS = 8


def shifted(value, axis, by):
    size = lax.axis_size(axis)
    return lax.ppermute(value, axis, [(i, (i + by) % size) for i in range(size)])


def exchanged(blocks, axes):
    return lax.all_to_all(blocks, axes, 0, 0, tiled=True)


def copies(value, count):
    return jnp.broadcast_to(value[None], (count, *value.shape))


def span_rows(first, second, shape):
    lane = lax.broadcasted_iota(jnp.int32, shape, 1)
    row = jnp.where(lane == 0, first, jnp.where(lane == 1, second, 0))
    return row.astype(jnp.float32).astype(jnp.bfloat16)


def project_kernel(zh_ref, odd_ref, span_ref, mine_ref, pair_ref, w_ref, out_ref):
    zh = zh_ref[0]
    odd = odd_ref[0]
    tokens = mine_ref.shape[2]
    places = w_ref.shape[1] // 2
    total = None
    for core in range(2):
        for place, (holder, block) in enumerate(((core, 0), (1, 1 + core), (core, 3), (0, 1 + core))):
            source = lax.rem(zh + place, places)
            w = w_ref[:, source * 2 + core]
            act = jnp.concatenate([mine_ref[holder, block], pair_ref[holder, block]], axis=0)
            part = jnp.dot(act, w.reshape(-1, w.shape[-1]), preferred_element_type=jnp.float32)
            total = part if total is None else total + part
    rounded = total.astype(out_ref.dtype)
    spans = span_rows(span_ref[0], span_ref[1], (SPAN_ROWS, total.shape[1]))
    for slot, rows in ((odd, rounded[:tokens]), (1 - odd, rounded[tokens:])):
        out_ref[slot, :tokens, :] = rows
        out_ref[slot, tokens:, :] = spans


def column_of(table, lane, place):
    return jnp.sum(jnp.where(lane == place, table, 0.0), axis=1, keepdims=True)


def attend_block(query, query_pos, kv_ref, pos_ref, top, total, mixed, factor):
    chunks = kv_ref.shape[0]
    width = query.shape[1]
    tokens = kv_ref.shape[4] - SPAN_ROWS
    count = kv_ref.shape[2] * 2 * tokens
    scores = []
    first = top
    for chunk in range(chunks):
        keys = kv_ref[chunk, 0, :, :, :tokens, :].reshape(count, width)
        score = lax.dot_general(
            query, keys, (((1,), (1,)), ((), ())), preferred_element_type=jnp.float32
        )
        score = jnp.where(pos_ref[chunk : chunk + 1, :] <= query_pos, score, HIDDEN)
        top = jnp.maximum(top, jnp.max(score, axis=1, keepdims=True))
        scores.append(score)
    if total is None:
        total = jnp.zeros(top.shape, jnp.float32)
        mixed = jnp.zeros(query.shape, jnp.float32)
    else:
        kept = jnp.exp2((first - top) * factor)
        total = total * kept
        mixed = mixed * kept
    for chunk in range(chunks):
        values = kv_ref[chunk, 1, :, :, :tokens, :].reshape(count, width)
        weight = jnp.exp2((scores[chunk] - top) * factor)
        total = total + jnp.sum(weight, axis=1, keepdims=True)
        mixed = mixed + jnp.dot(
            weight.astype(jnp.bfloat16), values, preferred_element_type=jnp.float32
        )
    return top, total, mixed


def fill_positions(kv_ref, pos_ref):
    chunks, _, lines = kv_ref.shape[:3]
    tokens = kv_ref.shape[4] - SPAN_ROWS
    half = tokens // 2
    count = lines * 2 * tokens
    lane = lax.broadcasted_iota(jnp.int32, (lines, count), 1)
    line = lax.broadcasted_iota(jnp.int32, (lines, count), 0)
    for chunk in range(chunks):
        total = jnp.zeros((1, count), jnp.float32)
        for slot in range(2):
            inside = lane - (line * 2 + slot) * tokens
            early = (inside >= 0) & (inside < half)
            late = (inside >= half) & (inside < tokens)
            held = kv_ref[chunk, slot, :, slot, tokens:, :].astype(jnp.float32)
            spans = jnp.max(held, axis=1) * half
            place = jnp.where(early, spans[:, 0:1], jnp.where(late, spans[:, 1:2] - half, 0.0))
            place = place + jnp.where(early | late, inside.astype(jnp.float32), 0.0)
            total = total + jnp.sum(place, axis=0, keepdims=True)
        pos_ref[chunk : chunk + 1, :] = total


def query_positions(q_ref, block, rows, tokens):
    half = tokens // 2
    row = lax.broadcasted_iota(jnp.int32, (tokens, 1), 0).astype(jnp.float32)
    spans = q_ref[block, rows : rows + SPAN_ROWS, :].astype(jnp.float32) * half
    query_pos = jnp.where(row < half, spans[0:1, 0:1], spans[0:1, 1:2] - half) + row
    return jnp.concatenate([query_pos] * (rows // tokens), axis=0)


def begin_kernel(q0_ref, q1_ref, q2_ref, q3_ref, kv_ref, mixed_ref, state_ref, pos_ref, q_ref, *, scale):
    for place, source_ref in enumerate((q0_ref, q1_ref, q2_ref, q3_ref)):
        q_ref[place] = source_ref[...]
    blocks = q_ref.shape[0]
    rows = q_ref.shape[1] - SPAN_ROWS
    factor = scale * math.log2(math.e)
    fill_positions(kv_ref, pos_ref)
    lane = lax.broadcasted_iota(jnp.int32, (rows, 128), 1)
    state_ref[...] = jnp.zeros(state_ref.shape, jnp.float32)

    def step(block, carry):
        query_pos = query_positions(q_ref, block, rows, kv_ref.shape[4] - SPAN_ROWS)
        top = jnp.full((rows, 1), FLOOR, jnp.float32)
        query = q_ref[block, :rows, :]
        top, total, mixed = attend_block(query, query_pos, kv_ref, pos_ref, top, None, None, factor)
        mixed_ref[block] = mixed
        state = jnp.where(lane == block, top, state_ref[...])
        state_ref[...] = jnp.where(lane == block + 8, total, state)
        return carry

    lax.fori_loop(0, blocks, step, 0)


def finish_kernel(
    own_ref, q0_ref, q1_ref, q2_ref, q3_ref, kv_ref, mixed_ref, state_ref,
    out_ref, stat_ref, pos_ref, q_ref, *, scale
):
    for place, source_ref in enumerate((q0_ref, q1_ref, q2_ref, q3_ref)):
        q_ref[place] = source_ref[...]
    own = own_ref[0]
    blocks = q_ref.shape[0]
    rows = q_ref.shape[1] - SPAN_ROWS
    factor = scale * math.log2(math.e)
    fill_positions(kv_ref, pos_ref)
    lane = lax.broadcasted_iota(jnp.int32, (rows, 128), 1)
    stat_ref[...] = jnp.zeros(stat_ref.shape, jnp.float32)

    def step(block, carry):
        owner = lax.rem(own + blocks - block, blocks)
        query_pos = query_positions(q_ref, block, rows, kv_ref.shape[4] - SPAN_ROWS)
        state = state_ref[...]
        top = column_of(state, lane, block)
        total = column_of(state, lane, block + 8)
        query = q_ref[block, :rows, :]
        top, total, mixed = attend_block(
            query, query_pos, kv_ref, pos_ref, top, total, mixed_ref[block], factor
        )
        seen = total > 0.0
        safe = jnp.where(seen, total, 1.0)
        out_ref[owner, :rows, :] = (mixed / safe).astype(jnp.bfloat16)
        size = jnp.where(seen, top * factor + jnp.log2(safe), HIDDEN)
        stat_ref[:rows, :] = jnp.where(lane == owner, size, stat_ref[:rows, :])
        return carry

    lax.fori_loop(0, blocks, step, 0)
    parts = []
    for chunk in range(stat_ref.shape[0] // 128):
        rest = stat_ref[chunk * 128 : (chunk + 1) * 128, :].T[:8]
        for third in range(3):
            high = rest.astype(jnp.bfloat16).astype(jnp.float32)
            parts.append((third * 4 + chunk, high))
            rest = rest - high
    place = lax.broadcasted_iota(jnp.int32, (STAT_ROWS, 128), 0)
    for block in range(blocks):
        tile = jnp.zeros((STAT_ROWS, 128), jnp.float32)
        for where, part in parts:
            tile = jnp.where(place == where, part[block : block + 1], tile)
        out_ref[block, rows:, :] = tile.astype(jnp.bfloat16)


def combine_kernel(in_ref, out_ref, total_ref, *, rows):
    blocks, _, width = in_ref.shape
    tokens = out_ref.shape[0]
    sizes = []
    for block in range(blocks):
        tile = in_ref[block, rows:, :].astype(jnp.float32)
        first = tile[:8]
        sizes.append(first + pltpu.roll(first, 4, 0) + tile[8:])
    top = sizes[0]
    for size in sizes[1:]:
        top = jnp.maximum(top, size)
    shares = [jnp.exp2(size - top) for size in sizes]
    whole = shares[0]
    for share in shares[1:]:
        whole = whole + share
    turned = jnp.concatenate([share / whole for share in shares], axis=0).T
    for start in range(0, rows, 128):
        count = min(128, rows - start)
        held = jnp.zeros((count, width), jnp.float32)
        for block in range(blocks):
            place = block * 8 + start // 128
            mixed = in_ref[block, start : start + count, :].astype(jnp.float32)
            held = held + turned[:count, place : place + 1] * mixed
        total_ref[start : start + count, :] = held
    for head in range(rows // tokens):
        kept = total_ref[head * tokens : (head + 1) * tokens, :]
        out_ref[:, head * width : (head + 1) * width] = kept.astype(out_ref.dtype)


VMEM = pl.BlockSpec()
SMEM = pl.BlockSpec(memory_space=pltpu.SMEM)


def body(activations, queries, w_kv, span_of):
    tokens, _ = activations.shape
    group, width = queries.shape[1:]
    rows = tokens * group
    ranks = lax.axis_size(HEADS)
    line = lax.axis_size(LINE)
    plane = lax.axis_size(PLANE)
    side = lax.axis_size("zi")
    zh = lax.axis_index("zh").astype(jnp.int32).reshape(1)
    odd = (lax.axis_index("x") % 2).astype(jnp.int32).reshape(1)
    own = lax.axis_index("zi").astype(jnp.int32).reshape(1)

    slabs = lax.axis_size("zh")
    turn = [(2 * i + c, 2 * ((i + 1 - 2 * c) % slabs) + c) for i in range(slabs) for c in range(2)]
    chip = lax.all_gather(activations, "core")
    near = lax.ppermute(chip, HEADS, turn)
    far = shifted(activations, "zh", 2)
    own_blocks = jnp.concatenate([activations[None], near, far[None]])
    pair_blocks = lax.ppermute(own_blocks, "x", [(i, i ^ 1) for i in range(lax.axis_size("x"))])
    mine = lax.all_gather(own_blocks, "core")
    pair = lax.all_gather(pair_blocks, "core")

    piece = w_kv.shape[0]
    w = w_kv.reshape(piece, ranks, 2 * width).transpose(1, 0, 2)
    w = exchanged(w, HEADS)
    w = exchanged(copies(w, line), LINE)
    w = w.transpose(1, 0, 2, 3).reshape(ranks, line * piece, 2 * width)
    parts = jnp.stack([w[..., :width], w[..., width:]])[None, :, None]
    parts = jnp.broadcast_to(parts, (lax.axis_size("x") // 2, 2, lax.axis_size("y"), *parts.shape[3:]))
    w = exchanged(parts.reshape(plane, *parts.shape[3:]), PLANE)

    spans = jnp.pad(span_of.astype(jnp.bfloat16)[None], ((0, SPAN_ROWS - 1), (0, width - 2)))
    q = queries.transpose(1, 0, 2).reshape(rows, width)
    q = jnp.concatenate([q, spans])
    moved = []
    for by in range(1, side):
        moved.append(shifted(q, "zi", by))

    kv = pl.pallas_call(
        project_kernel,
        out_shape=jax.ShapeDtypeStruct((2, tokens + SPAN_ROWS, width), jnp.bfloat16),
        in_specs=[SMEM, SMEM, SMEM, VMEM, VMEM, VMEM],
        out_specs=VMEM,
        name="project",
        compiler_params=pltpu.CompilerParams(vmem_limit_bytes=12 * 1024 * 1024),
    )(zh, odd, span_of, mine, pair, w)
    sets = (lax.axis_size("x") // 2, 2, lax.axis_size("y"), 2, tokens + SPAN_ROWS, width)
    other = shifted(kv, "zo", 1)
    first = exchanged(copies(kv, plane), PLANE).reshape(sets)
    spread = copies(other, plane)
    second = exchanged(spread, PLANE).reshape(sets)

    padded = (rows + 127) // 128 * 128
    scale = 1.0 / math.sqrt(width)
    positions = pltpu.VMEM((8, plane // 2 * tokens), jnp.float32)
    held = pltpu.VMEM((side, rows + SPAN_ROWS, width), jnp.bfloat16)
    mixed, state = pl.pallas_call(
        lambda *refs: begin_kernel(*refs, scale=scale),
        out_shape=(
            jax.ShapeDtypeStruct((side, rows, width), jnp.float32),
            jax.ShapeDtypeStruct((rows, 128), jnp.float32),
        ),
        in_specs=[VMEM] * 5,
        out_specs=(VMEM, VMEM),
        scratch_shapes=[positions, held],
        name="begin",
        compiler_params=pltpu.CompilerParams(vmem_limit_bytes=16 * 1024 * 1024),
    )(q, *moved, first)
    mixed = pl.pallas_call(
        lambda *refs: finish_kernel(*refs, scale=scale),
        out_shape=jax.ShapeDtypeStruct((side, rows + STAT_ROWS, width), jnp.bfloat16),
        in_specs=[SMEM] + [VMEM] * 7,
        out_specs=VMEM,
        scratch_shapes=[pltpu.VMEM((padded, 128), jnp.float32), positions, held],
        name="finish",
        compiler_params=pltpu.CompilerParams(vmem_limit_bytes=16 * 1024 * 1024),
    )(own, q, *moved, second, mixed, state)
    mixed = exchanged(mixed, "zi")
    return pl.pallas_call(
        lambda *refs: combine_kernel(*refs, rows=rows),
        out_shape=jax.ShapeDtypeStruct((tokens, group * width), jnp.bfloat16),
        in_specs=[VMEM],
        out_specs=VMEM,
        scratch_shapes=[pltpu.VMEM((rows, width), jnp.float32)],
        name="combine",
        compiler_params=pltpu.CompilerParams(vmem_limit_bytes=8 * 1024 * 1024),
    )(mixed)


def solution(mesh):
    finer = Mesh(mesh.devices.reshape(4, 2, 4, 4, 2, 4), ("zh", "core", "x", "y", "zo", "zi"))
    in_specs = (P(ROWS, HEADS), P(ROWS, HEADS, None), P(HEADS + ROWS, None, None, None), P(ROWS))
    return jax.shard_map(body, mesh=finer, in_specs=in_specs, out_specs=P(ROWS, HEADS), check_vma=False)
```

```python
import math

import jax
import jax.numpy as jnp
from jax import lax
from jax.experimental import pallas as pl
from jax.experimental.pallas import tpu as pltpu
from jax.sharding import Mesh
from jax.sharding import PartitionSpec as P


ROWS = ("x", "y", "zo", "zi")
HEADS = ("zh", "core")
PLANE = ("x", "y")
LINE = ("zo", "zi")
HIDDEN = -1e30
FLOOR = -1e29
STAT_ROWS = 16
SPAN_ROWS = 8


def shifted(value, axis, by):
    size = lax.axis_size(axis)
    return lax.ppermute(value, axis, [(i, (i + by) % size) for i in range(size)])


def exchanged(blocks, axes):
    return lax.all_to_all(blocks, axes, 0, 0, tiled=True)


def copies(value, count):
    return jnp.broadcast_to(value[None], (count, *value.shape))


def span_rows(first, second, shape):
    lane = lax.broadcasted_iota(jnp.int32, shape, 1)
    row = jnp.where(lane == 0, first, jnp.where(lane == 1, second, 0))
    return row.astype(jnp.float32).astype(jnp.bfloat16)


def project_kernel(zh_ref, odd_ref, span_ref, mine_ref, pair_ref, w_ref, out_ref):
    zh = zh_ref[0]
    odd = odd_ref[0]
    tokens = mine_ref.shape[2]
    places = w_ref.shape[1] // 2
    total = None
    for core in range(2):
        for place, (holder, block) in enumerate(((core, 0), (1, 1 + core), (core, 3), (0, 1 + core))):
            source = lax.rem(zh + place, places)
            w = w_ref[:, source * 2 + core]
            act = jnp.concatenate([mine_ref[holder, block], pair_ref[holder, block]], axis=0)
            part = jnp.dot(act, w.reshape(-1, w.shape[-1]), preferred_element_type=jnp.float32)
            total = part if total is None else total + part
    rounded = total.astype(out_ref.dtype)
    spans = span_rows(span_ref[0], span_ref[1], (SPAN_ROWS, total.shape[1]))
    for slot, rows in ((odd, rounded[:tokens]), (1 - odd, rounded[tokens:])):
        out_ref[slot, :tokens, :] = rows
        out_ref[slot, tokens:, :] = spans


def column_of(table, lane, place):
    return jnp.sum(jnp.where(lane == place, table, 0.0), axis=1, keepdims=True)


def attend_block(query, query_pos, kv_ref, pos_ref, top, total, mixed, factor):
    chunks = kv_ref.shape[0]
    width = query.shape[1]
    tokens = kv_ref.shape[4] - SPAN_ROWS
    count = kv_ref.shape[2] * 2 * tokens
    scores = []
    first = top
    for chunk in range(chunks):
        keys = kv_ref[chunk, 0, :, :, :tokens, :].reshape(count, width)
        score = lax.dot_general(
            query, keys, (((1,), (1,)), ((), ())), preferred_element_type=jnp.float32
        )
        score = jnp.where(pos_ref[chunk : chunk + 1, :] <= query_pos, score, HIDDEN)
        top = jnp.maximum(top, jnp.max(score, axis=1, keepdims=True))
        scores.append(score)
    if total is None:
        total = jnp.zeros(top.shape, jnp.float32)
        mixed = jnp.zeros(query.shape, jnp.float32)
    else:
        kept = jnp.exp2((first - top) * factor)
        total = total * kept
        mixed = mixed * kept
    for chunk in range(chunks):
        values = kv_ref[chunk, 1, :, :, :tokens, :].reshape(count, width)
        weight = jnp.exp2((scores[chunk] - top) * factor)
        total = total + jnp.sum(weight, axis=1, keepdims=True)
        mixed = mixed + jnp.dot(
            weight.astype(jnp.bfloat16), values, preferred_element_type=jnp.float32
        )
    return top, total, mixed


def fill_positions(kv_ref, pos_ref):
    chunks, _, lines = kv_ref.shape[:3]
    tokens = kv_ref.shape[4] - SPAN_ROWS
    half = tokens // 2
    count = lines * 2 * tokens
    lane = lax.broadcasted_iota(jnp.int32, (lines, count), 1)
    line = lax.broadcasted_iota(jnp.int32, (lines, count), 0)
    for chunk in range(chunks):
        total = jnp.zeros((1, count), jnp.float32)
        for slot in range(2):
            inside = lane - (line * 2 + slot) * tokens
            early = (inside >= 0) & (inside < half)
            late = (inside >= half) & (inside < tokens)
            held = kv_ref[chunk, slot, :, slot, tokens:, :].astype(jnp.float32)
            spans = jnp.max(held, axis=1) * half
            place = jnp.where(early, spans[:, 0:1], jnp.where(late, spans[:, 1:2] - half, 0.0))
            place = place + jnp.where(early | late, inside.astype(jnp.float32), 0.0)
            total = total + jnp.sum(place, axis=0, keepdims=True)
        pos_ref[chunk : chunk + 1, :] = total


def query_positions(q_ref, block, rows, tokens):
    half = tokens // 2
    row = lax.broadcasted_iota(jnp.int32, (tokens, 1), 0).astype(jnp.float32)
    spans = q_ref[block, rows : rows + SPAN_ROWS, :].astype(jnp.float32) * half
    query_pos = jnp.where(row < half, spans[0:1, 0:1], spans[0:1, 1:2] - half) + row
    return jnp.concatenate([query_pos] * (rows // tokens), axis=0)


def begin_kernel(q0_ref, q1_ref, q2_ref, q3_ref, kv_ref, mixed_ref, state_ref, pos_ref, q_ref, *, scale):
    for place, source_ref in enumerate((q0_ref, q1_ref, q2_ref, q3_ref)):
        q_ref[place] = source_ref[...]
    blocks = q_ref.shape[0]
    rows = q_ref.shape[1] - SPAN_ROWS
    factor = scale * math.log2(math.e)
    fill_positions(kv_ref, pos_ref)
    lane = lax.broadcasted_iota(jnp.int32, (rows, 128), 1)
    state_ref[...] = jnp.zeros(state_ref.shape, jnp.float32)

    def step(block, carry):
        query_pos = query_positions(q_ref, block, rows, kv_ref.shape[4] - SPAN_ROWS)
        top = jnp.full((rows, 1), FLOOR, jnp.float32)
        query = q_ref[block, :rows, :]
        top, total, mixed = attend_block(query, query_pos, kv_ref, pos_ref, top, None, None, factor)
        mixed_ref[block] = mixed
        state = jnp.where(lane == block, top, state_ref[...])
        state_ref[...] = jnp.where(lane == block + 8, total, state)
        return carry

    lax.fori_loop(0, blocks, step, 0)


def finish_kernel(
    own_ref, q0_ref, q1_ref, q2_ref, q3_ref, kv_ref, mixed_ref, state_ref,
    out_ref, stat_ref, pos_ref, q_ref, *, scale
):
    for place, source_ref in enumerate((q0_ref, q1_ref, q2_ref, q3_ref)):
        q_ref[place] = source_ref[...]
    own = own_ref[0]
    blocks = q_ref.shape[0]
    rows = q_ref.shape[1] - SPAN_ROWS
    factor = scale * math.log2(math.e)
    fill_positions(kv_ref, pos_ref)
    lane = lax.broadcasted_iota(jnp.int32, (rows, 128), 1)
    stat_ref[...] = jnp.zeros(stat_ref.shape, jnp.float32)

    def step(block, carry):
        owner = lax.rem(own + blocks - block, blocks)
        query_pos = query_positions(q_ref, block, rows, kv_ref.shape[4] - SPAN_ROWS)
        state = state_ref[...]
        top = column_of(state, lane, block)
        total = column_of(state, lane, block + 8)
        query = q_ref[block, :rows, :]
        top, total, mixed = attend_block(
            query, query_pos, kv_ref, pos_ref, top, total, mixed_ref[block], factor
        )
        seen = total > 0.0
        safe = jnp.where(seen, total, 1.0)
        out_ref[owner, :rows, :] = (mixed / safe).astype(jnp.bfloat16)
        size = jnp.where(seen, top * factor + jnp.log2(safe), HIDDEN)
        stat_ref[:rows, :] = jnp.where(lane == owner, size, stat_ref[:rows, :])
        return carry

    lax.fori_loop(0, blocks, step, 0)
    parts = []
    for chunk in range(stat_ref.shape[0] // 128):
        rest = stat_ref[chunk * 128 : (chunk + 1) * 128, :].T[:8]
        for third in range(3):
            high = rest.astype(jnp.bfloat16).astype(jnp.float32)
            parts.append((third * 4 + chunk, high))
            rest = rest - high
    place = lax.broadcasted_iota(jnp.int32, (STAT_ROWS, 128), 0)
    for block in range(blocks):
        tile = jnp.zeros((STAT_ROWS, 128), jnp.float32)
        for where, part in parts:
            tile = jnp.where(place == where, part[block : block + 1], tile)
        out_ref[block, rows:, :] = tile.astype(jnp.bfloat16)


def combine_kernel(in_ref, out_ref, total_ref, *, rows):
    blocks, _, width = in_ref.shape
    tokens = out_ref.shape[0]
    sizes = []
    for block in range(blocks):
        tile = in_ref[block, rows:, :].astype(jnp.float32)
        first = tile[:8]
        sizes.append(first + pltpu.roll(first, 4, 0) + tile[8:])
    top = sizes[0]
    for size in sizes[1:]:
        top = jnp.maximum(top, size)
    shares = [jnp.exp2(size - top) for size in sizes]
    whole = shares[0]
    for share in shares[1:]:
        whole = whole + share
    turned = jnp.concatenate([share / whole for share in shares], axis=0).T
    for start in range(0, rows, 128):
        count = min(128, rows - start)
        held = jnp.zeros((count, width), jnp.float32)
        for block in range(blocks):
            place = block * 8 + start // 128
            mixed = in_ref[block, start : start + count, :].astype(jnp.float32)
            held = held + turned[:count, place : place + 1] * mixed
        total_ref[start : start + count, :] = held
    for head in range(rows // tokens):
        kept = total_ref[head * tokens : (head + 1) * tokens, :]
        out_ref[:, head * width : (head + 1) * width] = kept.astype(out_ref.dtype)


VMEM = pl.BlockSpec()
SMEM = pl.BlockSpec(memory_space=pltpu.SMEM)


def body(activations, queries, w_kv, span_of):
    tokens, _ = activations.shape
    group, width = queries.shape[1:]
    rows = tokens * group
    ranks = lax.axis_size(HEADS)
    line = lax.axis_size(LINE)
    plane = lax.axis_size(PLANE)
    side = lax.axis_size("zi")
    zh = lax.axis_index("zh").astype(jnp.int32).reshape(1)
    odd = (lax.axis_index("x") % 2).astype(jnp.int32).reshape(1)
    own = lax.axis_index("zi").astype(jnp.int32).reshape(1)

    slabs = lax.axis_size("zh")
    turn = [(2 * i + c, 2 * ((i + 1 - 2 * c) % slabs) + c) for i in range(slabs) for c in range(2)]
    chip = lax.all_gather(activations, "core")
    near = lax.ppermute(chip, HEADS, turn)
    far = shifted(activations, "zh", 2)
    swap = [(i, i ^ 1) for i in range(lax.axis_size("x"))]
    first_blocks = jnp.concatenate([activations[None], near])
    pair_near = lax.ppermute(first_blocks, "x", swap)
    pair_far = lax.ppermute(far, "x", swap)
    mine = lax.all_gather(jnp.concatenate([first_blocks, far[None]]), "core")
    pair = lax.all_gather(jnp.concatenate([pair_near, pair_far[None]]), "core")

    piece = w_kv.shape[0]
    w = w_kv.reshape(piece, ranks, 2 * width).transpose(1, 0, 2)
    w = exchanged(w, HEADS)
    w = exchanged(copies(w, line), LINE)
    w = w.transpose(1, 0, 2, 3).reshape(ranks, line * piece, 2 * width)
    parts = jnp.stack([w[..., :width], w[..., width:]])[None, :, None]
    parts = jnp.broadcast_to(parts, (lax.axis_size("x") // 2, 2, lax.axis_size("y"), *parts.shape[3:]))
    w = exchanged(parts.reshape(plane, *parts.shape[3:]), PLANE)

    spans = jnp.pad(span_of.astype(jnp.bfloat16)[None], ((0, SPAN_ROWS - 1), (0, width - 2)))
    q = queries.transpose(1, 0, 2).reshape(rows, width)
    q = jnp.concatenate([q, spans])
    moved = []
    for by in range(1, side):
        moved.append(shifted(q, "zi", by))

    kv = pl.pallas_call(
        project_kernel,
        out_shape=jax.ShapeDtypeStruct((2, tokens + SPAN_ROWS, width), jnp.bfloat16),
        in_specs=[SMEM, SMEM, SMEM, VMEM, VMEM, VMEM],
        out_specs=VMEM,
        name="project",
        compiler_params=pltpu.CompilerParams(vmem_limit_bytes=12 * 1024 * 1024),
    )(zh, odd, span_of, mine, pair, w)
    sets = (lax.axis_size("x") // 2, 2, lax.axis_size("y"), 2, tokens + SPAN_ROWS, width)
    other = shifted(kv, "zo", 1)
    first = exchanged(copies(kv, plane), PLANE).reshape(sets)
    spread = copies(other, plane)
    second = exchanged(spread, PLANE).reshape(sets)

    padded = (rows + 127) // 128 * 128
    scale = 1.0 / math.sqrt(width)
    positions = pltpu.VMEM((8, plane // 2 * tokens), jnp.float32)
    held = pltpu.VMEM((side, rows + SPAN_ROWS, width), jnp.bfloat16)
    mixed, state = pl.pallas_call(
        lambda *refs: begin_kernel(*refs, scale=scale),
        out_shape=(
            jax.ShapeDtypeStruct((side, rows, width), jnp.float32),
            jax.ShapeDtypeStruct((rows, 128), jnp.float32),
        ),
        in_specs=[VMEM] * 5,
        out_specs=(VMEM, VMEM),
        scratch_shapes=[positions, held],
        name="begin",
        compiler_params=pltpu.CompilerParams(vmem_limit_bytes=16 * 1024 * 1024),
    )(q, *moved, first)
    mixed = pl.pallas_call(
        lambda *refs: finish_kernel(*refs, scale=scale),
        out_shape=jax.ShapeDtypeStruct((side, rows + STAT_ROWS, width), jnp.bfloat16),
        in_specs=[SMEM] + [VMEM] * 7,
        out_specs=VMEM,
        scratch_shapes=[pltpu.VMEM((padded, 128), jnp.float32), positions, held],
        name="finish",
        compiler_params=pltpu.CompilerParams(vmem_limit_bytes=16 * 1024 * 1024),
    )(own, q, *moved, second, mixed, state)
    mixed = exchanged(mixed, "zi")
    return pl.pallas_call(
        lambda *refs: combine_kernel(*refs, rows=rows),
        out_shape=jax.ShapeDtypeStruct((tokens, group * width), jnp.bfloat16),
        in_specs=[VMEM],
        out_specs=VMEM,
        scratch_shapes=[pltpu.VMEM((rows, width), jnp.float32)],
        name="combine",
        compiler_params=pltpu.CompilerParams(vmem_limit_bytes=8 * 1024 * 1024),
    )(mixed)


def solution(mesh):
    finer = Mesh(mesh.devices.reshape(4, 2, 4, 4, 2, 4), ("zh", "core", "x", "y", "zo", "zi"))
    in_specs = (P(ROWS, HEADS), P(ROWS, HEADS, None), P(HEADS + ROWS, None, None, None), P(ROWS))
    return jax.shard_map(body, mesh=finer, in_specs=in_specs, out_specs=P(ROWS, HEADS), check_vma=False)
```
